32 devices in a mesh: vocab: 16 (over z, x, core), seq: 2 (over y).
Axes of the slice: x: 2, y: 2, z: 4, core: 2. Of those that a mesh axis runs over, the one named last changes fastest.
Arguments:
- hidden_states: bfloat16 [512, 3584], P('seq', 'vocab'), may hold values from -6 to 6
- norm_gain: float32 [3584], replicated, may hold values from 0.5 to 1.5
- embedding: bfloat16 [256000, 3584], P(('vocab', 'seq')), may hold values from -0.29882812 to 0.29882812
- targets: int32 [512], replicated, may hold values from 0 to 255999
Outputs:
- token_loss: float32 [512], P('seq')
- mean_loss: float32 [], replicated
The draws below stay inside these ranges and needn't reach their ends.
All inputs are finite; a program needn't handle non-finite values.
Results may differ from the reference program's by a relative error of at most 0.0005.
Values may be sent and summed in bfloat16 or wider, within the bound.
A program may use at most 128 MiB of HBM per device.

```python
import jax
import jax.numpy as jnp
from jax import lax

D = 3584
VOCAB = 256000
TOKENS = 512
N_VOCAB = 16


def place_ends(values, own_key, smallest, largest):
    longest = values.shape.index(max(values.shape))
    spots = []
    for shift in (0, 1):
        where = [jax.random.randint(jax.random.fold_in(own_key, axis), (), 0, length) for axis, length in enumerate(values.shape)]
        where[longest] = (where[longest] + shift) % values.shape[longest]
        spots.append(tuple(where))
    return values.at[spots[0]].set(smallest).at[spots[1]].set(largest)


def block_scale(key, shape, cuts, least, high):
    def one(dim, blocks):
        steps = jax.random.uniform(jax.random.fold_in(jax.random.fold_in(key, 6), dim), (blocks,), jnp.float32, least / len(cuts), high / len(cuts))
        return jnp.repeat(jnp.exp(steps), shape[dim] // blocks).reshape((-1,) + (1,) * (len(shape) - dim - 1))

    level = one(*cuts[0])
    for cut in cuts[1:]:
        level = level * one(*cut)
    return level


def scatter_about(rng, extent, deviation, reach, split=(), held_as=jnp.bfloat16):
    drawn = jax.random.normal(rng, extent, jnp.float32) * deviation
    if len(split) > 0:
        drawn = block_scale(rng, extent, split, -0.22, 0.18) * drawn
    return jnp.clip(drawn, min=-reach, max=reach).astype(held_as)


def setup_inputs(seed: int = 0) -> dict:
    seeds = jax.random.split(jax.random.key(seed), 5)
    return {
        "hidden_states": scatter_about(seeds[0], (TOKENS, D), 1.0, 6.0, ((0, 2), (1, 16))),
        "norm_gain": jnp.clip(1.0 + 0.1 * jax.random.normal(seeds[1], (D,), jnp.float32), 0.5, 1.5),
        "embedding": scatter_about(seeds[2], (VOCAB, D), (3.0 * D ** -0.5), 0.29882812, ((0, 32),)),
        "targets": place_ends(jax.random.randint(seeds[3], (TOKENS,), 0, VOCAB), jax.random.fold_in(seeds[3], 1), 0, VOCAB - 1).astype(jnp.int32),
    }


def reference(hidden_states, norm_gain, embedding, targets):
    values = hidden_states.astype(jnp.float32)
    meansq = lax.optimization_barrier(jnp.mean(values * values, axis=-1, keepdims=True))
    normed = (values * lax.rsqrt(meansq + 1e-06) * norm_gain).astype(jnp.bfloat16)
    block_rows = VOCAB // N_VOCAB
    blocks = embedding.reshape(N_VOCAB, block_rows, D)
    starts = jnp.arange(N_VOCAB, dtype=jnp.int32) * block_rows

    def visit(carry, inputs):
        total, picked = carry
        table, start = inputs
        scores = jnp.dot(table, normed.T, preferred_element_type=jnp.float32)
        capped = 30.0 * jnp.tanh(scores / 30.0)
        total = total + lax.optimization_barrier(jnp.sum(jnp.exp(capped), axis=0))
        ids = start + jnp.arange(block_rows, dtype=jnp.int32)
        hit = ids[:, None] == targets[None, :]
        picked = picked + lax.optimization_barrier(jnp.sum(jnp.where(hit, capped, 0.0), axis=0))
        return ((total, picked), None)
    zeros = jnp.zeros((TOKENS,), jnp.float32)
    (total, picked), unused = lax.scan(visit, (zeros, zeros), (blocks, starts))
    token_loss = jnp.log(total) - picked
    return (token_loss, jnp.mean(token_loss))
```

```python
import functools

import jax
import jax.numpy as jnp
from jax import lax
from jax.experimental import pallas as pl
from jax.experimental.pallas import tpu as pltpu
from jax.sharding import PartitionSpec as P

LANES = 128
MXU = 256
UNROLL = 2
LOG2E = 1.4426950408889634


def block_rows(rows, limit):
    return max(n for n in range(16, limit + 1, 16) if rows % n == 0)


def cut_phases(planes, gw):
    ends = [(k + 1) * gw // MXU * MXU for k in range(planes)]
    ends[-1] = planes * gw
    return [(a, b - a) for a, b in zip([0] + ends[:-1], ends)]


def kernel(cfg, ht_ref, gain_ref, targets_ref, emb_ref, loss_ref, mean_ref,
           raw, zbuf, normed, acc, area_a, area_b, gcol, stat, rbuf, fin, lossbuf,
           sums, z_send, z_recv, p_send, p_recv, c_send, c_recv, s_send, s_recv,
           f_send, f_recv, own_sem, e_sem):
    nv, ns, group, planes, width, own, tokens, rows, padded, bm, features = cfg
    v, s = lax.axis_index("vocab"), lax.axis_index("seq")
    p, q = v // group, v % group
    core = q % 2
    half = (group // 2) * ns
    hidx = (q // 2) * ns + s
    count = nv * ns
    me = s * nv + v
    gw = group * width
    phases = cut_phases(planes, gw)
    nblk = padded // bm
    lanes_of = lambda i: pl.ds(pl.multiple_of(i * LANES, LANES), LANES)

    def plane_of(k):
        return (p + planes - k) % planes

    def loop(low, high, action):
        def body(i, _):
            action(i)
            return 0
        lax.fori_loop(low, high, body, 0)

    def area(ph):
        return area_a if ph % 2 == 0 else area_b

    def table_copies(ph):
        first, size = phases[ph]
        copies, at = [], first
        while at < first + size:
            k = at // gw
            end = min((k + 1) * gw, first + size)
            col = pl.multiple_of(plane_of(k) * gw + at % gw, LANES)
            copies.append(pltpu.make_async_copy(
                emb_ref.at[:, pl.ds(col, end - at)],
                area(ph).at[pl.ds(0, rows), pl.ds(at - first, end - at)],
                e_sem.at[ph, len(copies)]))
            at = end
        return copies

    def fetch(ph):
        for copy in table_copies(ph):
            copy.start()

    def fetched(ph):
        for copy in table_copies(ph):
            copy.wait()

    def peer_of(e):
        dp, rest = e // (group * ns), e % (group * ns)
        return (((p + planes - dp) % planes) * group + (q + rest // ns) % group,
                (s + rest % ns) % ns)

    barrier = pltpu.get_barrier_semaphore()

    def greet(e):
        vv, ss = peer_of(e)
        pl.semaphore_signal(barrier, inc=1, device_id={"vocab": vv, "seq": ss},
                            device_id_type=pl.DeviceIdType.MESH)

    loop(1, count, greet)
    fetch(0)
    if len(phases) > 1:
        fetch(1)
    h = ht_ref[...].astype(jnp.float32)
    stat[me] = jnp.sum(h * h, axis=0, keepdims=True)
    pl.semaphore_wait(barrier, count - 1)

    def remote(src, dst, send, recv, vv, ss):
        return pltpu.make_async_remote_copy(
            src_ref=src, dst_ref=dst, send_sem=send, recv_sem=recv,
            device_id={"vocab": vv, "seq": ss},
            device_id_type=pl.DeviceIdType.MESH)

    def tile_at(k, qq, ss):
        place = raw if k == 0 else normed
        row = 0 if k == 0 else k * gw
        return place.at[pl.ds(pl.multiple_of(row + qq * width, 16), width),
                        pl.ds(pl.multiple_of(ss * own, LANES), own)]

    def own_of(k):
        return ht_ref if k == 0 else tile_at(k, q, s)

    def z_copy(k):
        return remote(ht_ref, zbuf.at[k - 1], z_send.at[k], z_recv.at[k],
                      (p + k) % planes * group + q, s)

    def p_copy(k, j):
        other = (hidx + j) % half
        return remote(own_of(k), tile_at(k, q, s), p_send.at[k, j], p_recv.at[k, j],
                      p * group + 2 * (other // ns) + core, other % ns)

    def c_copy(k, j):
        tile = (hidx + half - j) % half
        place = tile_at(k, 2 * (tile // ns) + core, tile % ns)
        return remote(place, place, c_send.at[k, j], c_recv.at[k, j],
                      p * group + (q + 1 - 2 * core), s)

    def c_own(k):
        return remote(own_of(k), tile_at(k, q, s), c_send.at[k, 0], c_recv.at[k, 0],
                      p * group + (q + 1 - 2 * core), s)

    def s_copy(e):
        return remote(stat.at[me], stat.at[me], s_send.at[e], s_recv.at[e], *peer_of(e))

    def spread(k):
        loop(1, half, lambda j: p_copy(k, j).start())
        c_own(k).start()

    def relay(k):
        def one(j):
            p_copy(k, j).wait_recv()
            c_copy(k, j).start()
        loop(1, half, one)

    def gathered(k):
        loop(0, half, lambda j: c_copy(k, j).wait_recv())

    loop(1, count, lambda e: s_copy(e).start())
    spread(0)
    for k in range(1, planes):
        z_copy(k).start()
    own_copy = pltpu.make_async_copy(ht_ref, tile_at(0, q, s), own_sem)
    own_copy.start()

    for k in range(planes):
        for i in range(gw // LANES):
            row = plane_of(k) * (gw // LANES) + i
            gcol[k * gw + i * LANES:k * gw + (i + 1) * LANES, :] = jnp.broadcast_to(
                gain_ref[pl.ds(row, 1), :], (LANES, LANES)).T
    sums[...] = jnp.zeros_like(sums)
    if padded > rows:
        for area_ref in (area_a, area_b):
            area_ref[rows // 16 * 16:, :] = jnp.zeros(
                (padded - rows // 16 * 16, area_ref.shape[1]), jnp.bfloat16)

    relay(0)
    loop(1, count, lambda e: s_copy(e).wait_recv())
    for t in range(ns):
        meansq = jnp.sum(stat[t * nv:(t + 1) * nv], axis=0) / features
        rbuf[:, t * own:(t + 1) * own] = lax.rsqrt(meansq + 1e-06)

    def ready(k):
        z_copy(k).wait_recv()
        place = tile_at(k, q, s)
        for c in range(own // LANES):
            scale = rbuf[:, lanes_of(s * (own // LANES) + c)]
            values = zbuf[k - 1, :, c * LANES:(c + 1) * LANES].astype(jnp.float32)
            gain = gcol[pl.ds(pl.multiple_of(k * gw + q * width, 16), width), :]
            place[:, c * LANES:(c + 1) * LANES] = (values * scale * gain).astype(jnp.bfloat16)
        spread(k)

    def run(*held):
        cols_of = [list(range(c, min(c + 2, tokens // MXU))) for c in range(0, tokens // MXU, 2)]
        accs = [held[0:2], held[2:4]]

        def push(ph, cols, i, reg):
            at = phases[ph][0] + i * MXU
            for m, c in enumerate(cols):
                pltpu.matmul_push_rhs(
                    normed[at:at + MXU, c * MXU:(c + 1) * MXU],
                    staging_register=reg, mxu_index=m)

        def feed(ph, cols, block, turn, seq, more):
            passes = phases[ph][1] // MXU
            place = pl.ds(pl.multiple_of(block * bm, 16), bm)
            for i in range(passes):
                reg = (seq + i) % 2
                part = area(ph)[place, i * MXU:(i + 1) * MXU]
                for m, _ in enumerate(cols):
                    pltpu.matmul_acc_lhs(accs[turn][m], part, load_staged_rhs=reg)
                if i + 1 < passes:
                    push(ph, cols, i + 1, 1 - reg)
                elif more:
                    push(ph, cols, 0, 1 - reg)
            return seq + passes

        base = (v * ns + s) * rows

        def drain(ph, cols, block, turn):
            place = pl.ds(pl.multiple_of(block * bm, 8), bm)
            for m, c in enumerate(cols):
                lane = slice(c * MXU, (c + 1) * MXU)
                scores = pltpu.matmul_pop(accs[turn][m])
                if ph > 0:
                    scores = scores + acc[place, lane]
                if ph + 1 < len(phases):
                    acc[place, lane] = scores
                    continue
                bent = jnp.tanh(scores * (1.0 / 30.0))
                grown = jnp.exp2(bent * (30.0 * LOG2E))
                want = targets_ref[:, lane] - (base + block * bm)
                index = lax.broadcasted_iota(jnp.int32, (bm, MXU), 0)
                hit = index == want
                if padded > rows:
                    real = index < rows - block * bm
                    hit = hit & real
                    grown = jnp.where(real, grown, 0.0)
                mine = jnp.where(hit, bent, 0.0)
                sums[0:8, lane] += jnp.sum(grown.reshape(bm // 8, 8, MXU), axis=0)
                sums[8:16, lane] += jnp.sum(mine.reshape(bm // 8, 8, MXU), axis=0)

        def phase(ph, cols, events):
            passes = phases[ph][1] // MXU
            trips = max(nblk - 2, 0) // UNROLL
            push(ph, cols, 0, 0)
            feed(ph, cols, 0, 0, 0, nblk > 1)

            def trip(j):
                seq = passes
                for u in range(UNROLL):
                    block = 1 + j * UNROLL + u
                    seq = feed(ph, cols, block, (1 + u) % 2, seq, True)
                    drain(ph, cols, block - 1, u % 2)

            done = 0
            rest = list(range(1 + trips * UNROLL, nblk))
            assert rest or nblk == 1
            for at, action in sorted(events, key=lambda event: event[0]):
                stop = int(at * trips)
                if stop > done:
                    loop(done, stop, trip)
                    done = stop
                action()
            if trips > done:
                loop(done, trips, trip)
            seq = passes * (1 + trips * UNROLL)
            for block in rest:
                seq = feed(ph, cols, block, block % 2, seq, block + 1 < nblk)
                drain(ph, cols, block - 1, (block - 1) % 2)
            drain(ph, cols, nblk - 1, (nblk - 1) % 2)

        for turn in range(2):
            for m in range(2):
                blank = jnp.zeros((bm, MXU), jnp.bfloat16)
                pltpu.matmul_acc_lhs(accs[turn][m], blank, load_staged_rhs=turn)
                pltpu.matmul_pop(accs[turn][m])

        events = [[] for _ in range(planes + 1)]
        for k in range(2, planes):
            events[0].append(((k - 1) / planes, functools.partial(ready, k)))
        for k in range(1, planes):
            when = 0.8 if k == 1 else 0.6
            events[k - 1].append((when, functools.partial(relay, k)))
        for ph in range(len(phases)):
            if ph > 0:
                gathered(ph)
                if ph + 1 < len(phases):
                    fetch(ph + 1)
            fetched(ph)
            for g, cols in enumerate(cols_of):
                phase(ph, cols, events[ph] if g == 0 else [])

    if planes > 1:
        ready(1)
    own_copy.wait()
    gathered(0)
    for i in range(gw // LANES):
        part = slice(i * LANES, (i + 1) * LANES)
        for c in range(tokens // LANES):
            cols = slice(c * LANES, (c + 1) * LANES)
            out = raw[part, cols].astype(jnp.float32) * rbuf[:, cols] * gcol[part, :]
            normed[part, cols] = out.astype(jnp.bfloat16)

    pl.run_scoped(run, *(pltpu.ACC(m)((bm, MXU), jnp.float32)
                         for _ in range(2) for m in range(2)))

    def f_copy(e):
        return remote(fin.at[me], fin.at[me], f_send.at[e], f_recv.at[e], *peer_of(e))

    fin[me, 0:1, :] = jnp.sum(sums[0:8, :], axis=0, keepdims=True)
    fin[me, 1:2, :] = jnp.sum(sums[8:16, :], axis=0, keepdims=True)
    loop(1, count, lambda e: f_copy(count - e).start())
    loop(1, count, lambda e: f_copy(e).wait_recv())
    both = jnp.sum(fin[...], axis=0)
    losses = jnp.log(both[0:1, :]) - 30.0 * both[1:2, :]
    lossbuf[...] = losses
    mean_ref[...] = jnp.sum(losses, axis=1, keepdims=True) / tokens
    loss_ref[...] = lossbuf[:, pl.ds(pl.multiple_of(s * own, LANES), own)]

    loop(1, count, lambda e: s_copy(e).wait_send())
    for k in range(planes):
        if k > 0:
            z_copy(k).wait_send()
        loop(1, half, lambda j: p_copy(k, j).wait_send())
        loop(0, half, lambda j: c_copy(k, j).wait_send())
    loop(1, count, lambda e: f_copy(e).wait_send())


def local(nv, ns, hidden_states, norm_gain, embedding, targets):
    own, width = hidden_states.shape
    rows, features = embedding.shape
    tokens = targets.shape[0]
    group = 2
    while (group * width) % LANES:
        group *= 2
    planes = nv // group
    gw = group * width
    padded = -(-rows // 16) * 16
    bm = block_rows(padded, 400)
    half = (group // 2) * ns
    count = nv * ns
    phases = cut_phases(planes, gw)
    cfg = (nv, ns, group, planes, width, own, tokens, rows, padded, bm, features)
    dma = pltpu.SemaphoreType.DMA
    vmem = pl.BlockSpec(memory_space=pltpu.VMEM)
    loss, mean = pl.pallas_call(
        functools.partial(kernel, cfg),
        out_shape=(jax.ShapeDtypeStruct((1, own), jnp.float32),
                   jax.ShapeDtypeStruct((1, 1), jnp.float32)),
        in_specs=[vmem, vmem, vmem, pl.BlockSpec(memory_space=pl.ANY)],
        out_specs=(vmem, vmem),
        scratch_shapes=[
            pltpu.VMEM((gw, tokens), jnp.bfloat16),
            pltpu.VMEM((max(planes - 1, 1), width, own), jnp.bfloat16),
            pltpu.VMEM((features, tokens), jnp.bfloat16),
            pltpu.VMEM((padded, tokens), jnp.float32),
            pltpu.VMEM((padded, max(n for _, n in phases[0::2])), jnp.bfloat16),
            pltpu.VMEM((padded, max(n for _, n in phases[1::2] or [(0, LANES)])), jnp.bfloat16),
            pltpu.VMEM((features, LANES), jnp.float32),
            pltpu.VMEM((count, 1, own), jnp.float32),
            pltpu.VMEM((1, tokens), jnp.float32),
            pltpu.VMEM((count, 2, tokens), jnp.float32),
            pltpu.VMEM((1, tokens), jnp.float32),
            pltpu.VMEM((16, tokens), jnp.float32),
            dma((planes,)), dma((planes,)),
            dma((planes, half)), dma((planes, half)),
            dma((planes, half)), dma((planes, half)),
            dma((count,)), dma((count,)),
            dma((count,)), dma((count,)),
            dma, dma((len(phases), 2)),
        ],
        compiler_params=pltpu.CompilerParams(
            collective_id=0, has_side_effects=True, vmem_limit_bytes=60 * 2**20),
    )(hidden_states.T, norm_gain.reshape(-1, LANES), targets.reshape(1, -1), embedding)
    return loss.reshape(own), mean.reshape(())


def solution(mesh):
    placed = (P("seq", "vocab"), P(), P(("vocab", "seq"), None), P())
    body = functools.partial(local, mesh.shape["vocab"], mesh.shape["seq"])
    return jax.shard_map(
        body, mesh=mesh, in_specs=placed, out_specs=(P("seq"), P()), check_vma=False
    )
```

```python
import functools

import jax
import jax.numpy as jnp
from jax import lax
from jax.experimental import pallas as pl
from jax.experimental.pallas import tpu as pltpu
from jax.sharding import PartitionSpec as P

LANES = 128
MXU = 256
UNROLL = 2
LAG = 2
READY = (0.0, 0.0, 0.9, 0.34)
RELAY = (0.0, 0.78, 0.9, 0.78)
LOG2E = 1.4426950408889634


def block_rows(rows, limit):
    return max(n for n in range(16, limit + 1, 16) if rows % n == 0)


def cut_phases(planes, gw):
    ends = [(k + 1) * gw // MXU * MXU for k in range(planes)]
    ends[-1] = planes * gw
    return [(a, b - a) for a, b in zip([0] + ends[:-1], ends)]


def kernel(cfg, ht_ref, gain_ref, targets_ref, emb_ref, loss_ref, mean_ref,
           raw, zbuf, normed, acc, area_a, area_b, gcol, chain, stat, rbuf, fin, lossbuf,
           sums, z_send, z_recv, p_send, p_recv, c_send, c_recv, s_send, s_recv,
           f_send, f_recv, d_send, d_recv, own_sem, e_sem):
    nv, ns, group, planes, width, own, tokens, rows, padded, bm, features = cfg
    v, s = lax.axis_index("vocab"), lax.axis_index("seq")
    p, q = v // group, v % group
    core = q % 2
    half = (group // 2) * ns
    hidx = (q // 2) * ns + s
    count = nv * ns
    me = s * nv + v
    mine_at = s * group + q
    gw = group * width
    raws = min(2, planes)
    phases = cut_phases(planes, gw)
    nblk = padded // bm
    lanes_of = lambda i: pl.ds(pl.multiple_of(i * LANES, LANES), LANES)

    def plane_of(k):
        return (p + planes - k) % planes

    def loop(low, high, action):
        def body(i, _):
            action(i)
            return 0
        lax.fori_loop(low, high, body, 0)

    def area(ph):
        return area_a if ph % 2 == 0 else area_b

    def table_copies(ph):
        first, size = phases[ph]
        copies, at = [], first
        while at < first + size:
            k = at // gw
            end = min((k + 1) * gw, first + size)
            col = pl.multiple_of(plane_of(k) * gw + at % gw, LANES)
            copies.append(pltpu.make_async_copy(
                emb_ref.at[:, pl.ds(col, end - at)],
                area(ph).at[pl.ds(0, rows), pl.ds(at - first, end - at)],
                e_sem.at[ph, len(copies)]))
            at = end
        return copies

    def fetch(ph):
        for copy in table_copies(ph):
            copy.start()

    def fetched(ph):
        for copy in table_copies(ph):
            copy.wait()

    def peer_of(e):
        dp, rest = e // (group * ns), e % (group * ns)
        return (((p + planes - dp) % planes) * group + (q + rest // ns) % group,
                (s + rest % ns) % ns)

    barrier = pltpu.get_barrier_semaphore()

    def greet(e):
        vv, ss = peer_of(e)
        pl.semaphore_signal(barrier, inc=1, device_id={"vocab": vv, "seq": ss},
                            device_id_type=pl.DeviceIdType.MESH)

    def few(low, high, action):
        if high - low > 32:
            loop(low, high, action)
        else:
            for i in range(low, high):
                action(i)

    chain[...] = jnp.zeros_like(chain)
    few(1, group * ns, greet)

    def call(pp):
        pl.semaphore_signal(barrier, inc=1, device_id={"vocab": pp * group + q, "seq": s},
                            device_id_type=pl.DeviceIdType.MESH)

    @pl.when(p > 0)
    def _():
        call(p - 1)

    @pl.when(p + 1 < planes)
    def _():
        call(p + 1)

    h = ht_ref[...].astype(jnp.float32)
    chain[2] = jnp.sum(h * h, axis=0, keepdims=True)
    beside = (p > 0).astype(jnp.int32) + (p + 1 < planes).astype(jnp.int32)
    pl.semaphore_wait(barrier, group * ns - 1 + beside)

    def remote(src, dst, send, recv, vv, ss):
        return pltpu.make_async_remote_copy(
            src_ref=src, dst_ref=dst, send_sem=send, recv_sem=recv,
            device_id={"vocab": vv, "seq": ss},
            device_id_type=pl.DeviceIdType.MESH)

    def tile_at(k, qq, ss):
        place = raw if k < raws else normed
        row = k * gw
        return place.at[pl.ds(pl.multiple_of(row + qq * width, 16), width),
                        pl.ds(pl.multiple_of(ss * own, LANES), own)]

    def own_of(k):
        return ht_ref if k == 0 else tile_at(k, q, s)

    def up():
        return remote(chain.at[3], chain.at[0], d_send.at[0], d_recv.at[0],
                      (p + 1) * group + q, s)

    def down():
        return remote(chain.at[4], chain.at[1], d_send.at[1], d_recv.at[1],
                      (p - 1) * group + q, s)

    def pass_up():
        chain[3] = chain[2] + chain[0]

        @pl.when(p + 1 < planes)
        def _():
            up().start()

    def pass_down():
        chain[4] = chain[2] + chain[1]

        @pl.when(p > 0)
        def _():
            down().start()

    def z_copy(k):
        place = tile_at(k, q, s) if k < raws else zbuf.at[k - raws]
        return remote(ht_ref, place, z_send.at[k], z_recv.at[k],
                      (p + k) % planes * group + q, s)

    def p_copy(k, j):
        other = (hidx + j) % half
        return remote(own_of(k), tile_at(k, q, s), p_send.at[k, j], p_recv.at[k, j],
                      p * group + 2 * (other // ns) + core, other % ns)

    def c_copy(k, j):
        tile = (hidx + half - j) % half
        place = tile_at(k, 2 * (tile // ns) + core, tile % ns)
        return remote(place, place, c_send.at[k, j], c_recv.at[k, j],
                      p * group + (q + 1 - 2 * core), s)

    def c_own(k):
        return remote(own_of(k), tile_at(k, q, s), c_send.at[k, 0], c_recv.at[k, 0],
                      p * group + (q + 1 - 2 * core), s)

    def s_copy(e):
        return remote(stat.at[mine_at], stat.at[mine_at], s_send.at[e], s_recv.at[e], *peer_of(e))

    def spread(k):
        loop(1, half, lambda j: p_copy(k, j).start())
        c_own(k).start()

    def relay(k):
        def one(j):
            p_copy(k, j).wait_recv()
            c_copy(k, j).start()
        loop(1, half, one)

    def gathered(k):
        loop(0, half, lambda j: c_copy(k, j).wait_recv())

    @pl.when(p == 0)
    def _():
        pass_up()

    @pl.when(p == planes - 1)
    def _():
        pass_down()

    spread(0)
    own_copy = pltpu.make_async_copy(ht_ref, tile_at(0, q, s), own_sem)
    own_copy.start()

    @pl.when(p > 0)
    def _():
        up().wait_recv()
        pass_up()

    @pl.when(p + 1 < planes)
    def _():
        down().wait_recv()
        pass_down()

    stat[mine_at] = chain[0] + chain[1] + chain[2]
    few(1, group * ns, lambda e: s_copy(e).start())
    for k in range(1, planes):
        z_copy(k).start()

    for k in range(planes):
        for i in range(gw // LANES):
            row = plane_of(k) * (gw // LANES) + i
            gcol[k * gw + i * LANES:k * gw + (i + 1) * LANES, :] = jnp.broadcast_to(
                gain_ref[pl.ds(row, 1), :], (LANES, LANES)).T
    sums[...] = jnp.zeros_like(sums)
    if padded > rows:
        for area_ref in (area_a, area_b):
            area_ref[rows // 16 * 16:, :] = jnp.zeros(
                (padded - rows // 16 * 16, area_ref.shape[1]), jnp.bfloat16)

    def ready(k):
        z_copy(k).wait_recv()
        place = tile_at(k, q, s)
        for c in range(own // LANES if k >= raws else 0):
            scale = rbuf[:, lanes_of(s * (own // LANES) + c)]
            values = zbuf[k - raws, :, c * LANES:(c + 1) * LANES].astype(jnp.float32)
            gain = gcol[pl.ds(pl.multiple_of(k * gw + q * width, 16), width), :]
            place[:, c * LANES:(c + 1) * LANES] = (values * scale * gain).astype(jnp.bfloat16)
        spread(k)

    def normalize(k):
        for i in range(k * gw // LANES, (k + 1) * gw // LANES):
            part = slice(i * LANES, (i + 1) * LANES)
            for c in range(tokens // LANES):
                cols = slice(c * LANES, (c + 1) * LANES)
                out = raw[part, cols].astype(jnp.float32) * rbuf[:, cols] * gcol[part, :]
                normed[part, cols] = out.astype(jnp.bfloat16)

    fetch(0)
    if len(phases) > 1:
        fetch(1)
    relay(0)
    if planes > 1:
        ready(1)
    few(1, group * ns, lambda e: s_copy(e).wait_recv())
    for t in range(ns):
        meansq = jnp.sum(stat[t * group:(t + 1) * group], axis=0) / features
        rbuf[:, t * own:(t + 1) * own] = lax.rsqrt(meansq + 1e-06)

    def run(*held):
        cols_of = [list(range(c, min(c + 2, tokens // MXU))) for c in range(0, tokens // MXU, 2)]
        accs = [held[0:2], held[2:4]]

        def push(ph, cols, i, reg):
            at = phases[ph][0] + i * MXU
            for m, c in enumerate(cols):
                pltpu.matmul_push_rhs(
                    normed[at:at + MXU, c * MXU:(c + 1) * MXU],
                    staging_register=reg, mxu_index=m)

        def feed(ph, cols, block, turn, seq, more):
            passes = phases[ph][1] // MXU
            place = pl.ds(pl.multiple_of(block * bm, 16), bm)
            for i in range(passes):
                reg = (seq + i) % 2
                part = area(ph)[place, i * MXU:(i + 1) * MXU]
                for m, _ in enumerate(cols):
                    pltpu.matmul_acc_lhs(accs[turn][m], part, load_staged_rhs=reg)
                if i + 1 < passes:
                    push(ph, cols, i + 1, 1 - reg)
                elif more:
                    push(ph, cols, 0, 1 - reg)
            return seq + passes

        base = (v * ns + s) * rows

        def drain(ph, cols, block, turn):
            place = pl.ds(pl.multiple_of(block * bm, 8), bm)
            for m, c in enumerate(cols):
                lane = slice(c * MXU, (c + 1) * MXU)
                scores = pltpu.matmul_pop(accs[turn][m])
                if ph > 0:
                    scores = scores + acc[place, lane]
                acc[place, lane] = scores

        def finish(cols, block):
            for c in cols:
                lane = slice(c * MXU, (c + 1) * MXU)
                want = (targets_ref[:, lane] - (base + block * bm)
                        - lax.broadcasted_iota(jnp.int32, (8, MXU), 0))
                total, picked = sums[0:8, lane], sums[8:16, lane]
                for r in range(0, bm, 8):
                    place = pl.ds(pl.multiple_of(block * bm + r, 8), 8)
                    bent = jnp.tanh(acc[place, lane] * (1.0 / 30.0))
                    grown = jnp.exp2(bent * (30.0 * LOG2E))
                    hit = want == r
                    if padded > rows:
                        real = block * bm + r < rows
                        hit = hit & real
                        grown = jnp.where(real, grown, 0.0)
                    picked = jnp.where(hit, bent, picked)
                    total = total + grown
                sums[0:8, lane], sums[8:16, lane] = total, picked

        def phase(ph, cols, events):
            passes = phases[ph][1] // MXU
            last = ph + 1 == len(phases)
            lead = min(LAG if last else 1, nblk)
            trips = max(nblk - 1 - lead, 0) // UNROLL

            def step(block, turn, seq, more, behind):
                seq = feed(ph, cols, block, turn, seq, more)
                if last and behind >= LAG:
                    finish(cols, block - LAG)
                if behind > 0:
                    drain(ph, cols, block - 1, 1 - turn)
                return seq

            push(ph, cols, 0, 0)
            seq = 0
            for block in range(lead):
                seq = step(block, block % 2, seq, block + 1 < nblk, block)

            def trip(j):
                seq = passes * lead
                for u in range(UNROLL):
                    seq = step(lead + j * UNROLL + u, (lead + u) % 2, seq, True, lead)

            done = 0
            for at, action in sorted(events, key=lambda event: event[0]):
                stop = int(at * trips)
                if stop > done:
                    loop(done, stop, trip)
                    done = stop
                action()
            if trips > done:
                loop(done, trips, trip)
            for block in range(lead + trips * UNROLL, nblk):
                seq = step(block, block % 2, passes * block, block + 1 < nblk, block)
            drain(ph, cols, nblk - 1, (nblk - 1) % 2)
            for block in range(max(nblk - LAG, 0), nblk) if last else ():
                finish(cols, block)

        for turn in range(2):
            for m in range(2):
                blank = jnp.zeros((bm, MXU), jnp.bfloat16)
                pltpu.matmul_acc_lhs(accs[turn][m], blank, load_staged_rhs=turn)
                pltpu.matmul_pop(accs[turn][m])

        events = [[] for _ in range(planes + 1)]
        for k in range(2, planes):
            events[max(k - 2, 0)].append((READY[min(k, 3)], functools.partial(ready, k)))
        for k in range(1, planes):
            events[k - 1].append((RELAY[min(k, 3)], functools.partial(relay, k)))
        for ph in range(len(phases)):
            if ph > 0:
                gathered(ph)
                if ph < raws:
                    normalize(ph)
                if ph + 1 < len(phases):
                    fetch(ph + 1)
            fetched(ph)
            for g, cols in enumerate(cols_of):
                phase(ph, cols, events[ph] if g == 0 else [])

    own_copy.wait()
    gathered(0)
    normalize(0)

    pl.run_scoped(run, *(pltpu.ACC(m)((bm, MXU), jnp.float32)
                         for _ in range(2) for m in range(2)))

    def f_copy(e):
        return remote(fin.at[me], fin.at[me], f_send.at[e], f_recv.at[e], *peer_of(e))

    fin[me, 0:1, :] = jnp.sum(sums[0:8, :], axis=0, keepdims=True)
    fin[me, 1:2, :] = jnp.sum(sums[8:16, :], axis=0, keepdims=True)
    few(1, count, lambda e: f_copy(count - e).start())
    loop(1, group * ns, lambda e: s_copy(e).wait_send())
    @pl.when(p + 1 < planes)
    def _():
        up().wait_send()

    @pl.when(p > 0)
    def _():
        down().wait_send()

    for k in range(planes):
        if k > 0:
            z_copy(k).wait_send()
        loop(1, half, lambda j: p_copy(k, j).wait_send())
        loop(0, half, lambda j: c_copy(k, j).wait_send())
    loop(1, count, lambda e: f_copy(e).wait_send())
    loop(1, count, lambda e: f_copy(e).wait_recv())
    both = jnp.sum(fin[...], axis=0)
    losses = jnp.log(both[0:1, :]) - 30.0 * both[1:2, :]
    lossbuf[...] = losses
    mean_ref[...] = jnp.sum(losses, axis=1, keepdims=True) / tokens
    loss_ref[...] = lossbuf[:, pl.ds(pl.multiple_of(s * own, LANES), own)]


def local(nv, ns, hidden_states, norm_gain, embedding, targets):
    own, width = hidden_states.shape
    rows, features = embedding.shape
    tokens = targets.shape[0]
    group = 2
    while (group * width) % LANES:
        group *= 2
    planes = nv // group
    gw = group * width
    padded = -(-rows // 16) * 16
    bm = block_rows(padded, 400)
    half = (group // 2) * ns
    count = nv * ns
    phases = cut_phases(planes, gw)
    cfg = (nv, ns, group, planes, width, own, tokens, rows, padded, bm, features)
    dma = pltpu.SemaphoreType.DMA
    vmem = pl.BlockSpec(memory_space=pltpu.VMEM)
    loss, mean = pl.pallas_call(
        functools.partial(kernel, cfg),
        out_shape=(pltpu.VMEM((1, own), jnp.float32), pltpu.VMEM((1, 1), jnp.float32)),
        in_specs=[vmem, vmem, vmem, pl.BlockSpec(memory_space=pl.ANY)],
        out_specs=(vmem, vmem),
        scratch_shapes=[
            pltpu.VMEM((min(2, planes) * gw, tokens), jnp.bfloat16),
            pltpu.VMEM((max(planes - 2, 1), width, own), jnp.bfloat16),
            pltpu.VMEM((features, tokens), jnp.bfloat16),
            pltpu.VMEM((padded, tokens), jnp.float32),
            pltpu.VMEM((padded, max(n for _, n in phases[0::2])), jnp.bfloat16),
            pltpu.VMEM((padded, max(n for _, n in phases[1::2] or [(0, LANES)])), jnp.bfloat16),
            pltpu.VMEM((features, LANES), jnp.float32),
            pltpu.VMEM((5, 1, own), jnp.float32),
            pltpu.VMEM((group * ns, 1, own), jnp.float32),
            pltpu.VMEM((1, tokens), jnp.float32),
            pltpu.VMEM((count, 2, tokens), jnp.float32),
            pltpu.VMEM((1, tokens), jnp.float32),
            pltpu.VMEM((16, tokens), jnp.float32),
            dma((planes,)), dma((planes,)),
            dma((planes, half)), dma((planes, half)),
            dma((planes, half)), dma((planes, half)),
            dma((group * ns,)), dma((group * ns,)),
            dma((count,)), dma((count,)),
            dma((2,)), dma((2,)),
            dma, dma((len(phases), 2)),
        ],
        compiler_params=pltpu.CompilerParams(
            collective_id=0, has_side_effects=True, vmem_limit_bytes=60 * 2**20),
    )(hidden_states.T, norm_gain.reshape(-1, LANES), targets.reshape(1, -1), embedding)
    return loss.reshape(own), mean.reshape(())


def solution(mesh):
    placed = (P("seq", "vocab"), P(), P(("vocab", "seq"), None), P())
    body = functools.partial(local, mesh.shape["vocab"], mesh.shape["seq"])
    return jax.shard_map(
        body, mesh=mesh, in_specs=placed, out_specs=(P("seq"), P()), check_vma=False
    )
```

```python
import functools

import jax
import jax.numpy as jnp
from jax import lax
from jax.experimental import pallas as pl
from jax.experimental.pallas import tpu as pltpu
from jax.sharding import PartitionSpec as P

LANES = 128
MXU = 256
UNROLL = 2
LAST_UNROLL = 8
LAG = 2
READY = (0.0, 0.0, 0.9, 0.34)
RELAY = (0.0, 0.78, 0.9, 0.78)
LOG2E = 1.4426950408889634


def block_rows(rows, limit):
    return max(n for n in range(16, limit + 1, 16) if rows % n == 0)


def cut_phases(planes, gw):
    ends = [(k + 1) * gw // MXU * MXU for k in range(planes)]
    ends[-1] = planes * gw
    return [(a, b - a) for a, b in zip([0] + ends[:-1], ends)]


def kernel(cfg, ht_ref, gain_ref, targets_ref, emb_ref, loss_ref, mean_ref,
           raw, zbuf, normed, acc, area_a, area_b, gcol, chain, stat, rbuf, fin, lossbuf,
           sums, z_send, z_recv, p_send, p_recv, c_send, c_recv, s_send, s_recv,
           f_send, f_recv, d_send, d_recv, own_sem, e_sem):
    nv, ns, group, planes, width, own, tokens, rows, padded, bm, features = cfg
    v, s = lax.axis_index("vocab"), lax.axis_index("seq")
    p, q = v // group, v % group
    core = q % 2
    half = (group // 2) * ns
    hidx = (q // 2) * ns + s
    count = nv * ns
    me = s * nv + v
    mine_at = s * group + q
    gw = group * width
    raws = min(2, planes)
    phases = cut_phases(planes, gw)
    nblk = padded // bm
    lanes_of = lambda i: pl.ds(pl.multiple_of(i * LANES, LANES), LANES)

    def plane_of(k):
        return (p + planes - k) % planes

    def loop(low, high, action):
        def body(i, _):
            action(i)
            return 0
        lax.fori_loop(low, high, body, 0)

    def area(ph):
        return area_a if ph % 2 == 0 else area_b

    def table_copies(ph):
        first, size = phases[ph]
        copies, at = [], first
        while at < first + size:
            k = at // gw
            end = min((k + 1) * gw, first + size)
            col = pl.multiple_of(plane_of(k) * gw + at % gw, LANES)
            copies.append(pltpu.make_async_copy(
                emb_ref.at[:, pl.ds(col, end - at)],
                area(ph).at[pl.ds(0, rows), pl.ds(at - first, end - at)],
                e_sem.at[ph, len(copies)]))
            at = end
        return copies

    def fetch(ph):
        for copy in table_copies(ph):
            copy.start()

    def fetched(ph):
        for copy in table_copies(ph):
            copy.wait()

    def peer_of(e):
        dp, rest = e // (group * ns), e % (group * ns)
        return (((p + planes - dp) % planes) * group + (q + rest // ns) % group,
                (s + rest % ns) % ns)

    barrier = pltpu.get_barrier_semaphore()

    def greet(e):
        vv, ss = peer_of(e)
        pl.semaphore_signal(barrier, inc=1, device_id={"vocab": vv, "seq": ss},
                            device_id_type=pl.DeviceIdType.MESH)

    def few(low, high, action):
        if high - low > 32:
            loop(low, high, action)
        else:
            for i in range(low, high):
                action(i)

    chain[...] = jnp.zeros_like(chain)
    few(1, group * ns, greet)

    def call(pp):
        pl.semaphore_signal(barrier, inc=1, device_id={"vocab": pp * group + q, "seq": s},
                            device_id_type=pl.DeviceIdType.MESH)

    @pl.when(p > 0)
    def _():
        call(p - 1)

    @pl.when(p + 1 < planes)
    def _():
        call(p + 1)

    fetch(0)
    if len(phases) > 1:
        fetch(1)
    h = ht_ref[...].astype(jnp.float32)
    chain[2] = jnp.sum(h * h, axis=0, keepdims=True)
    beside = (p > 0).astype(jnp.int32) + (p + 1 < planes).astype(jnp.int32)
    pl.semaphore_wait(barrier, group * ns - 1 + beside)

    def remote(src, dst, send, recv, vv, ss):
        return pltpu.make_async_remote_copy(
            src_ref=src, dst_ref=dst, send_sem=send, recv_sem=recv,
            device_id={"vocab": vv, "seq": ss},
            device_id_type=pl.DeviceIdType.MESH)

    def tile_at(k, qq, ss):
        place = raw if k < raws else normed
        row = k * gw
        return place.at[pl.ds(pl.multiple_of(row + qq * width, 16), width),
                        pl.ds(pl.multiple_of(ss * own, LANES), own)]

    def own_of(k):
        return ht_ref if k == 0 else tile_at(k, q, s)

    def up():
        return remote(chain.at[3], chain.at[0], d_send.at[0], d_recv.at[0],
                      (p + 1) * group + q, s)

    def down():
        return remote(chain.at[4], chain.at[1], d_send.at[1], d_recv.at[1],
                      (p - 1) * group + q, s)

    def pass_up():
        chain[3] = chain[2] + chain[0]

        @pl.when(p + 1 < planes)
        def _():
            up().start()

    def pass_down():
        chain[4] = chain[2] + chain[1]

        @pl.when(p > 0)
        def _():
            down().start()

    def z_copy(k):
        place = tile_at(k, q, s) if k < raws else zbuf.at[k - raws]
        return remote(ht_ref, place, z_send.at[k], z_recv.at[k],
                      (p + k) % planes * group + q, s)

    def p_copy(k, j):
        other = (hidx + j) % half
        return remote(own_of(k), tile_at(k, q, s), p_send.at[k, j], p_recv.at[k, j],
                      p * group + 2 * (other // ns) + core, other % ns)

    def c_copy(k, j):
        tile = (hidx + half - j) % half
        place = tile_at(k, 2 * (tile // ns) + core, tile % ns)
        return remote(place, place, c_send.at[k, j], c_recv.at[k, j],
                      p * group + (q + 1 - 2 * core), s)

    def c_own(k):
        return remote(own_of(k), tile_at(k, q, s), c_send.at[k, 0], c_recv.at[k, 0],
                      p * group + (q + 1 - 2 * core), s)

    def s_copy(e):
        return remote(stat.at[mine_at], stat.at[mine_at], s_send.at[e], s_recv.at[e], *peer_of(e))

    def spread(k):
        loop(1, half, lambda j: p_copy(k, j).start())
        c_own(k).start()

    def relay(k):
        def one(j):
            p_copy(k, j).wait_recv()
            c_copy(k, j).start()
        loop(1, half, one)

    def gathered(k):
        loop(0, half, lambda j: c_copy(k, j).wait_recv())

    @pl.when(p == 0)
    def _():
        pass_up()

    @pl.when(p == planes - 1)
    def _():
        pass_down()

    spread(0)
    own_copy = pltpu.make_async_copy(ht_ref, tile_at(0, q, s), own_sem)
    own_copy.start()

    @pl.when(p > 0)
    def _():
        up().wait_recv()
        pass_up()

    if planes > 1:
        @pl.when(p + 1 < planes)
        def _():
            z_copy(1).start()

    @pl.when(p + 1 < planes)
    def _():
        down().wait_recv()
        pass_down()

    stat[mine_at] = chain[0] + chain[1] + chain[2]
    few(1, group * ns, lambda e: s_copy(e).start())
    if planes > 1:
        @pl.when(p + 1 == planes)
        def _():
            z_copy(1).start()

    for k in range(2, planes):
        z_copy(k).start()

    for k in range(planes):
        for i in range(gw // LANES):
            row = plane_of(k) * (gw // LANES) + i
            gcol[k * gw + i * LANES:k * gw + (i + 1) * LANES, :] = jnp.broadcast_to(
                gain_ref[pl.ds(row, 1), :], (LANES, LANES)).T
    sums[...] = jnp.zeros_like(sums)
    if padded > rows:
        for area_ref in (area_a, area_b):
            area_ref[rows // 16 * 16:, :] = jnp.zeros(
                (padded - rows // 16 * 16, area_ref.shape[1]), jnp.bfloat16)

    def ready(k):
        z_copy(k).wait_recv()
        place = tile_at(k, q, s)
        for c in range(own // LANES if k >= raws else 0):
            scale = rbuf[:, lanes_of(s * (own // LANES) + c)]
            values = zbuf[k - raws, :, c * LANES:(c + 1) * LANES].astype(jnp.float32)
            gain = gcol[pl.ds(pl.multiple_of(k * gw + q * width, 16), width), :]
            place[:, c * LANES:(c + 1) * LANES] = (values * scale * gain).astype(jnp.bfloat16)
        spread(k)

    def normalize(k):
        for i in range(k * gw // LANES, (k + 1) * gw // LANES):
            part = slice(i * LANES, (i + 1) * LANES)
            for c in range(tokens // LANES):
                cols = slice(c * LANES, (c + 1) * LANES)
                out = raw[part, cols].astype(jnp.float32) * rbuf[:, cols] * gcol[part, :]
                normed[part, cols] = out.astype(jnp.bfloat16)

    relay(0)
    if planes > 1:
        ready(1)
    few(1, group * ns, lambda e: s_copy(e).wait_recv())
    for t in range(ns):
        meansq = jnp.sum(stat[t * group:(t + 1) * group], axis=0) / features
        rbuf[:, t * own:(t + 1) * own] = lax.rsqrt(meansq + 1e-06)

    def run(*held):
        cols_of = [list(range(c, min(c + 2, tokens // MXU))) for c in range(0, tokens // MXU, 2)]
        accs = [held[0:2], held[2:4]]

        def push(ph, cols, i, reg):
            at = phases[ph][0] + i * MXU
            for m, c in enumerate(cols):
                pltpu.matmul_push_rhs(
                    normed[at:at + MXU, c * MXU:(c + 1) * MXU],
                    staging_register=reg, mxu_index=m)

        def feed(ph, cols, block, turn, seq, more):
            passes = phases[ph][1] // MXU
            place = pl.ds(pl.multiple_of(block * bm, 16), bm)
            for i in range(passes):
                reg = (seq + i) % 2
                part = area(ph)[place, i * MXU:(i + 1) * MXU]
                for m, _ in enumerate(cols):
                    pltpu.matmul_acc_lhs(accs[turn][m], part, load_staged_rhs=reg)
                if i + 1 < passes:
                    push(ph, cols, i + 1, 1 - reg)
                elif more:
                    push(ph, cols, 0, 1 - reg)
            return seq + passes

        base = (v * ns + s) * rows

        def drain(ph, cols, block, turn):
            place = pl.ds(pl.multiple_of(block * bm, 8), bm)
            for m, c in enumerate(cols):
                lane = slice(c * MXU, (c + 1) * MXU)
                scores = pltpu.matmul_pop(accs[turn][m])
                if ph > 0:
                    scores = scores + acc[place, lane]
                acc[place, lane] = scores

        def finish(cols, block):
            for c in cols:
                lane = slice(c * MXU, (c + 1) * MXU)
                want = (targets_ref[:, lane] - (base + block * bm)
                        - lax.broadcasted_iota(jnp.int32, (8, MXU), 0))
                total, picked = sums[0:8, lane], sums[8:16, lane]
                for r in range(0, bm, 8):
                    place = pl.ds(pl.multiple_of(block * bm + r, 8), 8)
                    bent = jnp.tanh(acc[place, lane] * (1.0 / 30.0))
                    grown = jnp.exp2(bent * (30.0 * LOG2E))
                    hit = want == r
                    if padded > rows:
                        real = block * bm + r < rows
                        hit = hit & real
                        grown = jnp.where(real, grown, 0.0)
                    picked = jnp.where(hit, bent, picked)
                    total = total + grown
                sums[0:8, lane], sums[8:16, lane] = total, picked

        def phase(ph, cols, events):
            passes = phases[ph][1] // MXU
            last = ph + 1 == len(phases)
            lead = min(LAG if last else 1, nblk)
            unroll = LAST_UNROLL if last else UNROLL
            trips = max(nblk - 1 - lead, 0) // unroll

            def step(block, turn, seq, more, behind):
                seq = feed(ph, cols, block, turn, seq, more)
                if last and behind >= LAG:
                    finish(cols, block - LAG)
                if behind > 0:
                    drain(ph, cols, block - 1, 1 - turn)
                return seq

            push(ph, cols, 0, 0)
            seq = 0
            for block in range(lead):
                seq = step(block, block % 2, seq, block + 1 < nblk, block)

            def trip(j):
                seq = passes * lead
                for u in range(unroll):
                    seq = step(lead + j * unroll + u, (lead + u) % 2, seq, True, lead)

            done = 0
            for at, action in sorted(events, key=lambda event: event[0]):
                stop = int(at * trips)
                if stop > done:
                    loop(done, stop, trip)
                    done = stop
                action()
            if trips > done:
                loop(done, trips, trip)
            for block in range(lead + trips * unroll, nblk):
                seq = step(block, block % 2, passes * block, block + 1 < nblk, block)
            drain(ph, cols, nblk - 1, (nblk - 1) % 2)
            for block in range(max(nblk - LAG, 0), nblk) if last else ():
                finish(cols, block)

        for turn in range(2):
            for m in range(2):
                blank = jnp.zeros((bm, MXU), jnp.bfloat16)
                pltpu.matmul_acc_lhs(accs[turn][m], blank, load_staged_rhs=turn)
                pltpu.matmul_pop(accs[turn][m])

        events = [[] for _ in range(planes + 1)]
        for k in range(2, planes):
            events[max(k - 2, 0)].append((READY[min(k, 3)], functools.partial(ready, k)))
        for k in range(1, planes):
            events[k - 1].append((RELAY[min(k, 3)], functools.partial(relay, k)))
        for ph in range(len(phases)):
            if ph > 0:
                gathered(ph)
                if ph < raws:
                    normalize(ph)
                if ph + 1 < len(phases):
                    fetch(ph + 1)
            fetched(ph)
            for g, cols in enumerate(cols_of):
                phase(ph, cols, events[ph] if g == 0 else [])

    own_copy.wait()
    gathered(0)
    normalize(0)

    pl.run_scoped(run, *(pltpu.ACC(m)((bm, MXU), jnp.float32)
                         for _ in range(2) for m in range(2)))

    def f_copy(e):
        return remote(fin.at[me], fin.at[me], f_send.at[e], f_recv.at[e], *peer_of(e))

    fin[me, 0:1, :] = jnp.sum(sums[0:8, :], axis=0, keepdims=True)
    fin[me, 1:2, :] = jnp.sum(sums[8:16, :], axis=0, keepdims=True)
    few(1, count, lambda e: f_copy(count - e).start())
    loop(1, group * ns, lambda e: s_copy(e).wait_send())
    @pl.when(p + 1 < planes)
    def _():
        up().wait_send()

    @pl.when(p > 0)
    def _():
        down().wait_send()

    for k in range(planes):
        if k > 0:
            z_copy(k).wait_send()
        loop(1, half, lambda j: p_copy(k, j).wait_send())
        loop(0, half, lambda j: c_copy(k, j).wait_send())
    loop(1, count, lambda e: f_copy(e).wait_send())
    loop(1, count, lambda e: f_copy(e).wait_recv())
    both = jnp.sum(fin[...], axis=0)
    losses = jnp.log(both[0:1, :]) - 30.0 * both[1:2, :]
    lossbuf[...] = losses
    mean_ref[...] = jnp.sum(losses, axis=1, keepdims=True) / tokens
    loss_ref[...] = lossbuf[:, pl.ds(pl.multiple_of(s * own, LANES), own)]


def local(nv, ns, hidden_states, norm_gain, embedding, targets):
    own, width = hidden_states.shape
    rows, features = embedding.shape
    tokens = targets.shape[0]
    group = 2
    while (group * width) % LANES:
        group *= 2
    planes = nv // group
    gw = group * width
    padded = -(-rows // 16) * 16
    bm = block_rows(padded, 400)
    half = (group // 2) * ns
    count = nv * ns
    phases = cut_phases(planes, gw)
    cfg = (nv, ns, group, planes, width, own, tokens, rows, padded, bm, features)
    dma = pltpu.SemaphoreType.DMA
    vmem = pl.BlockSpec(memory_space=pltpu.VMEM)
    loss, mean = pl.pallas_call(
        functools.partial(kernel, cfg),
        out_shape=(pltpu.VMEM((1, own), jnp.float32), pltpu.VMEM((1, 1), jnp.float32)),
        in_specs=[vmem, vmem, vmem, pl.BlockSpec(memory_space=pl.ANY)],
        out_specs=(vmem, vmem),
        scratch_shapes=[
            pltpu.VMEM((min(2, planes) * gw, tokens), jnp.bfloat16),
            pltpu.VMEM((max(planes - 2, 1), width, own), jnp.bfloat16),
            pltpu.VMEM((features, tokens), jnp.bfloat16),
            pltpu.VMEM((padded, tokens), jnp.float32),
            pltpu.VMEM((padded, max(n for _, n in phases[0::2])), jnp.bfloat16),
            pltpu.VMEM((padded, max(n for _, n in phases[1::2] or [(0, LANES)])), jnp.bfloat16),
            pltpu.VMEM((features, LANES), jnp.float32),
            pltpu.VMEM((5, 1, own), jnp.float32),
            pltpu.VMEM((group * ns, 1, own), jnp.float32),
            pltpu.VMEM((1, tokens), jnp.float32),
            pltpu.VMEM((count, 2, tokens), jnp.float32),
            pltpu.VMEM((1, tokens), jnp.float32),
            pltpu.VMEM((16, tokens), jnp.float32),
            dma((planes,)), dma((planes,)),
            dma((planes, half)), dma((planes, half)),
            dma((planes, half)), dma((planes, half)),
            dma((group * ns,)), dma((group * ns,)),
            dma((count,)), dma((count,)),
            dma((2,)), dma((2,)),
            dma, dma((len(phases), 2)),
        ],
        compiler_params=pltpu.CompilerParams(
            collective_id=0, has_side_effects=True, vmem_limit_bytes=60 * 2**20),
    )(hidden_states.T, norm_gain.reshape(-1, LANES), targets.reshape(1, -1), embedding)
    return loss.reshape(own), mean.reshape(())


def solution(mesh):
    placed = (P("seq", "vocab"), P(), P(("vocab", "seq"), None), P())
    body = functools.partial(local, mesh.shape["vocab"], mesh.shape["seq"])
    return jax.shard_map(
        body, mesh=mesh, in_specs=placed, out_specs=(P("seq"), P()), check_vma=False
    )
```

```python
import functools

import jax
import jax.numpy as jnp
from jax import lax
from jax.experimental import pallas as pl
from jax.experimental.pallas import tpu as pltpu
from jax.sharding import PartitionSpec as P

LANES = 128
MXU = 256
UNROLL = 2
LAST_UNROLL = 8
LAG = 2
READY = (0.0, 0.0, 0.9, 0.34)
RELAY = (0.0, 0.78, 0.9, 0.78)
LOG2E = 1.4426950408889634


def block_rows(rows, limit):
    return max(n for n in range(16, limit + 1, 16) if rows % n == 0)


def cut_phases(planes, gw):
    ends = [(k + 1) * gw // MXU * MXU for k in range(planes)]
    ends[-1] = planes * gw
    return [(a, b - a) for a, b in zip([0] + ends[:-1], ends)]


def kernel(cfg, ht_ref, gain_ref, targets_ref, emb_ref, loss_ref, mean_ref,
           raw, zbuf, normed, acc, area_a, area_b, gcol, chain, stat, rbuf, fin, lossbuf,
           sums, z_send, z_recv, p_send, p_recv, c_send, c_recv, s_send, s_recv,
           f_send, f_recv, d_send, d_recv, own_sem, e_sem):
    nv, ns, group, planes, width, own, tokens, rows, padded, bm, features = cfg
    v, s = lax.axis_index("vocab"), lax.axis_index("seq")
    p, q = v // group, v % group
    core = q % 2
    half = (group // 2) * ns
    hidx = (q // 2) * ns + s
    count = nv * ns
    me = s * nv + v
    mine_at = s * group + q
    gw = group * width
    raws = min(2, planes)
    phases = cut_phases(planes, gw)
    nblk = padded // bm
    lanes_of = lambda i: pl.ds(pl.multiple_of(i * LANES, LANES), LANES)

    def plane_of(k):
        return (p + planes - k) % planes

    def loop(low, high, action):
        def body(i, _):
            action(i)
            return 0
        lax.fori_loop(low, high, body, 0)

    def area(ph):
        return area_a if ph % 2 == 0 else area_b

    def table_copies(ph):
        first, size = phases[ph]
        copies, at = [], first
        while at < first + size:
            k = at // gw
            end = min((k + 1) * gw, first + size)
            col = pl.multiple_of(plane_of(k) * gw + at % gw, LANES)
            copies.append(pltpu.make_async_copy(
                emb_ref.at[:, pl.ds(col, end - at)],
                area(ph).at[pl.ds(0, rows), pl.ds(at - first, end - at)],
                e_sem.at[ph, len(copies)]))
            at = end
        return copies

    def fetch(ph):
        for copy in table_copies(ph):
            copy.start()

    def fetched(ph):
        for copy in table_copies(ph):
            copy.wait()

    def peer_of(e):
        dp, rest = e // (group * ns), e % (group * ns)
        return (((p + planes - dp) % planes) * group + (q + rest // ns) % group,
                (s + rest % ns) % ns)

    barrier = pltpu.get_barrier_semaphore()

    def greet(e):
        vv, ss = peer_of(e)
        pl.semaphore_signal(barrier, inc=1, device_id={"vocab": vv, "seq": ss},
                            device_id_type=pl.DeviceIdType.MESH)

    def few(low, high, action):
        if high - low > 32:
            loop(low, high, action)
        else:
            for i in range(low, high):
                action(i)

    chain[...] = jnp.zeros_like(chain)
    few(1, group * ns, greet)

    def call(pp):
        pl.semaphore_signal(barrier, inc=1, device_id={"vocab": pp * group + q, "seq": s},
                            device_id_type=pl.DeviceIdType.MESH)

    @pl.when(p > 0)
    def _():
        call(p - 1)

    @pl.when(p + 1 < planes)
    def _():
        call(p + 1)

    fetch(0)
    if len(phases) > 1:
        fetch(1)
    h = ht_ref[...].astype(jnp.float32)
    chain[2] = jnp.sum(h * h, axis=0, keepdims=True)
    beside = (p > 0).astype(jnp.int32) + (p + 1 < planes).astype(jnp.int32)
    pl.semaphore_wait(barrier, group * ns - 1 + beside)

    def remote(src, dst, send, recv, vv, ss):
        return pltpu.make_async_remote_copy(
            src_ref=src, dst_ref=dst, send_sem=send, recv_sem=recv,
            device_id={"vocab": vv, "seq": ss},
            device_id_type=pl.DeviceIdType.MESH)

    def tile_at(k, qq, ss):
        place = raw if k < raws else normed
        row = k * gw
        return place.at[pl.ds(pl.multiple_of(row + qq * width, 16), width),
                        pl.ds(pl.multiple_of(ss * own, LANES), own)]

    def own_of(k):
        return ht_ref if k == 0 else tile_at(k, q, s)

    def up():
        return remote(chain.at[3], chain.at[0], d_send.at[0], d_recv.at[0],
                      (p + 1) * group + q, s)

    def down():
        return remote(chain.at[4], chain.at[1], d_send.at[1], d_recv.at[1],
                      (p - 1) * group + q, s)

    def pass_up():
        chain[3] = chain[2] + chain[0]

        @pl.when(p + 1 < planes)
        def _():
            up().start()

    def pass_down():
        chain[4] = chain[2] + chain[1]

        @pl.when(p > 0)
        def _():
            down().start()

    def z_copy(k):
        place = tile_at(k, q, s) if k < raws else zbuf.at[k - raws]
        return remote(ht_ref, place, z_send.at[k], z_recv.at[k],
                      (p + k) % planes * group + q, s)

    def p_copy(k, j):
        other = (hidx + j) % half
        return remote(own_of(k), tile_at(k, q, s), (p_send.at[k, j] if k == 0 else z_send.at[k]), p_recv.at[k, j],
                      p * group + 2 * (other // ns) + core, other % ns)

    def c_copy(k, j):
        tile = (hidx + half - j) % half
        place = tile_at(k, 2 * (tile // ns) + core, tile % ns)
        return remote(place, place, (c_send.at[k, j] if k == 0 else z_send.at[k]), c_recv.at[k, j],
                      p * group + (q + 1 - 2 * core), s)

    def c_own(k):
        return remote(own_of(k), tile_at(k, q, s), (c_send.at[k, 0] if k == 0 else z_send.at[k]), c_recv.at[k, 0],
                      p * group + (q + 1 - 2 * core), s)

    def s_copy(e):
        return remote(stat.at[mine_at], stat.at[mine_at], s_send.at[e], s_recv.at[e], *peer_of(e))

    def spread(k):
        loop(1, half, lambda j: p_copy(k, j).start())
        c_own(k).start()

    def relay(k):
        def one(j):
            p_copy(k, j).wait_recv()
            c_copy(k, j).start()
        loop(1, half, one)

    def gathered(k):
        loop(0, half, lambda j: c_copy(k, j).wait_recv())

    @pl.when(p == 0)
    def _():
        pass_up()

    @pl.when(p == planes - 1)
    def _():
        pass_down()

    spread(0)
    own_copy = pltpu.make_async_copy(ht_ref, tile_at(0, q, s), own_sem)
    own_copy.start()

    @pl.when(p > 0)
    def _():
        up().wait_recv()
        pass_up()

    if planes > 1:
        @pl.when(p + 1 < planes)
        def _():
            z_copy(1).start()

    @pl.when(p + 1 < planes)
    def _():
        down().wait_recv()
        pass_down()

    stat[mine_at] = chain[0] + chain[1] + chain[2]
    few(1, group * ns, lambda e: s_copy(e).start())
    if planes > 1:
        @pl.when(p + 1 == planes)
        def _():
            z_copy(1).start()

    for k in range(2, planes):
        z_copy(k).start()

    for k in range(planes):
        for i in range(gw // LANES):
            row = plane_of(k) * (gw // LANES) + i
            gcol[k * gw + i * LANES:k * gw + (i + 1) * LANES, :] = jnp.broadcast_to(
                gain_ref[pl.ds(row, 1), :], (LANES, LANES)).T
    sums[...] = jnp.zeros_like(sums)
    if padded > rows:
        for area_ref in (area_a, area_b):
            area_ref[rows // 16 * 16:, :] = jnp.zeros(
                (padded - rows // 16 * 16, area_ref.shape[1]), jnp.bfloat16)

    def ready(k):
        z_copy(k).wait_recv()
        place = tile_at(k, q, s)
        for c in range(own // LANES if k >= raws else 0):
            scale = rbuf[:, lanes_of(s * (own // LANES) + c)]
            values = zbuf[k - raws, :, c * LANES:(c + 1) * LANES].astype(jnp.float32)
            gain = gcol[pl.ds(pl.multiple_of(k * gw + q * width, 16), width), :]
            place[:, c * LANES:(c + 1) * LANES] = (values * scale * gain).astype(jnp.bfloat16)
        spread(k)

    def normalize(k):
        for i in range(k * gw // LANES, (k + 1) * gw // LANES):
            part = slice(i * LANES, (i + 1) * LANES)
            for c in range(tokens // LANES):
                cols = slice(c * LANES, (c + 1) * LANES)
                out = raw[part, cols].astype(jnp.float32) * rbuf[:, cols] * gcol[part, :]
                normed[part, cols] = out.astype(jnp.bfloat16)

    relay(0)
    if planes > 1:
        ready(1)
    few(1, group * ns, lambda e: s_copy(e).wait_recv())
    for t in range(ns):
        meansq = jnp.sum(stat[t * group:(t + 1) * group], axis=0) / features
        rbuf[:, t * own:(t + 1) * own] = lax.rsqrt(meansq + 1e-06)

    def run(*held):
        cols_of = [list(range(c, min(c + 2, tokens // MXU))) for c in range(0, tokens // MXU, 2)]
        accs = [held[0:2], held[2:4]]

        def push(ph, cols, i, reg):
            at = phases[ph][0] + i * MXU
            for m, c in enumerate(cols):
                pltpu.matmul_push_rhs(
                    normed[at:at + MXU, c * MXU:(c + 1) * MXU],
                    staging_register=reg, mxu_index=m)

        def feed(ph, cols, block, turn, seq, more):
            passes = phases[ph][1] // MXU
            place = pl.ds(pl.multiple_of(block * bm, 16), bm)
            for i in range(passes):
                reg = (seq + i) % 2
                part = area(ph)[place, i * MXU:(i + 1) * MXU]
                for m, _ in enumerate(cols):
                    pltpu.matmul_acc_lhs(accs[turn][m], part, load_staged_rhs=reg)
                if i + 1 < passes:
                    push(ph, cols, i + 1, 1 - reg)
                elif more:
                    push(ph, cols, 0, 1 - reg)
            return seq + passes

        base = (v * ns + s) * rows

        def drain(ph, cols, block, turn):
            place = pl.ds(pl.multiple_of(block * bm, 8), bm)
            for m, c in enumerate(cols):
                lane = slice(c * MXU, (c + 1) * MXU)
                scores = pltpu.matmul_pop(accs[turn][m])
                if ph > 0:
                    scores = scores + acc[place, lane]
                acc[place, lane] = scores

        def finish(cols, block):
            for c in cols:
                lane = slice(c * MXU, (c + 1) * MXU)
                want = (targets_ref[:, lane] - (base + block * bm)
                        - lax.broadcasted_iota(jnp.int32, (8, MXU), 0))
                total, picked = sums[0:8, lane], sums[8:16, lane]
                for r in range(0, bm, 8):
                    place = pl.ds(pl.multiple_of(block * bm + r, 8), 8)
                    bent = jnp.tanh(acc[place, lane] * (1.0 / 30.0))
                    grown = jnp.exp2(bent * (30.0 * LOG2E))
                    hit = want == r
                    if padded > rows:
                        real = block * bm + r < rows
                        hit = hit & real
                        grown = jnp.where(real, grown, 0.0)
                    picked = jnp.where(hit, bent, picked)
                    total = total + grown
                sums[0:8, lane], sums[8:16, lane] = total, picked

        def phase(ph, cols, events):
            passes = phases[ph][1] // MXU
            last = ph + 1 == len(phases)
            lead = min(LAG if last else 1, nblk)
            unroll = LAST_UNROLL if last else UNROLL
            trips = max(nblk - 1 - lead, 0) // unroll

            def step(block, turn, seq, more, behind):
                seq = feed(ph, cols, block, turn, seq, more)
                if last and behind >= LAG:
                    finish(cols, block - LAG)
                if behind > 0:
                    drain(ph, cols, block - 1, 1 - turn)
                return seq

            push(ph, cols, 0, 0)
            seq = 0
            for block in range(lead):
                seq = step(block, block % 2, seq, block + 1 < nblk, block)

            def trip(j):
                seq = passes * lead
                for u in range(unroll):
                    seq = step(lead + j * unroll + u, (lead + u) % 2, seq, True, lead)

            done = 0
            for at, action in sorted(events, key=lambda event: event[0]):
                stop = int(at * trips)
                if stop > done:
                    loop(done, stop, trip)
                    done = stop
                action()
            if trips > done:
                loop(done, trips, trip)
            for block in range(lead + trips * unroll, nblk):
                seq = step(block, block % 2, passes * block, block + 1 < nblk, block)
            drain(ph, cols, nblk - 1, (nblk - 1) % 2)
            for block in range(max(nblk - LAG, 0), nblk) if last else ():
                finish(cols, block)

        for turn in range(2):
            for m in range(2):
                blank = jnp.zeros((bm, MXU), jnp.bfloat16)
                pltpu.matmul_acc_lhs(accs[turn][m], blank, load_staged_rhs=turn)
                pltpu.matmul_pop(accs[turn][m])

        events = [[] for _ in range(planes + 1)]
        for k in range(2, planes):
            events[max(k - 2, 0)].append((READY[min(k, 3)], functools.partial(ready, k)))
        for k in range(1, planes):
            events[k - 1].append((RELAY[min(k, 3)], functools.partial(relay, k)))
        for ph in range(len(phases)):
            if ph > 0:
                gathered(ph)
                if ph < raws:
                    normalize(ph)
                if ph + 1 < len(phases):
                    fetch(ph + 1)
            fetched(ph)
            for g, cols in enumerate(cols_of):
                phase(ph, cols, events[ph] if g == 0 else [])

    own_copy.wait()
    gathered(0)
    normalize(0)

    pl.run_scoped(run, *(pltpu.ACC(m)((bm, MXU), jnp.float32)
                         for _ in range(2) for m in range(2)))

    def f_copy(e):
        return remote(fin.at[me], fin.at[me], f_send, f_recv, *peer_of(e))

    fin[me, 0:1, :] = jnp.sum(sums[0:8, :], axis=0, keepdims=True)
    fin[me, 1:2, :] = jnp.sum(sums[8:16, :], axis=0, keepdims=True)
    few(1, count, lambda e: f_copy(count - e).start())
    loop(1, group * ns, lambda e: s_copy(e).wait_send())
    @pl.when(p + 1 < planes)
    def _():
        up().wait_send()

    @pl.when(p > 0)
    def _():
        down().wait_send()

    loop(1, half, lambda j: p_copy(0, j).wait_send())
    loop(0, half, lambda j: c_copy(0, j).wait_send())
    for k in range(1, planes):
        whole = (raw if k < raws else normed).at[k * gw:(k + 1) * gw, :]
        remote(whole, whole, z_send.at[k], z_recv.at[k], *peer_of(1)).wait_send()
    others = fin.at[0:count - 1]
    shared = remote(others, others, f_send, f_recv, *peer_of(1))
    shared.wait_send()
    shared.wait_recv()
    both = jnp.sum(fin[...], axis=0)
    losses = jnp.log(both[0:1, :]) - 30.0 * both[1:2, :]
    lossbuf[...] = losses
    mean_ref[...] = jnp.sum(losses, axis=1, keepdims=True) / tokens
    loss_ref[...] = lossbuf[:, pl.ds(pl.multiple_of(s * own, LANES), own)]


def local(nv, ns, hidden_states, norm_gain, embedding, targets):
    own, width = hidden_states.shape
    rows, features = embedding.shape
    tokens = targets.shape[0]
    group = 2
    while (group * width) % LANES:
        group *= 2
    planes = nv // group
    gw = group * width
    padded = -(-rows // 16) * 16
    bm = block_rows(padded, 400)
    half = (group // 2) * ns
    count = nv * ns
    phases = cut_phases(planes, gw)
    cfg = (nv, ns, group, planes, width, own, tokens, rows, padded, bm, features)
    dma = pltpu.SemaphoreType.DMA
    vmem = pl.BlockSpec(memory_space=pltpu.VMEM)
    loss, mean = pl.pallas_call(
        functools.partial(kernel, cfg),
        out_shape=(pltpu.VMEM((1, own), jnp.float32), pltpu.VMEM((1, 1), jnp.float32)),
        in_specs=[vmem, vmem, vmem, pl.BlockSpec(memory_space=pl.ANY)],
        out_specs=(vmem, vmem),
        scratch_shapes=[
            pltpu.VMEM((min(2, planes) * gw, tokens), jnp.bfloat16),
            pltpu.VMEM((max(planes - 2, 1), width, own), jnp.bfloat16),
            pltpu.VMEM((features, tokens), jnp.bfloat16),
            pltpu.VMEM((padded, tokens), jnp.float32),
            pltpu.VMEM((padded, max(n for _, n in phases[0::2])), jnp.bfloat16),
            pltpu.VMEM((padded, max(n for _, n in phases[1::2] or [(0, LANES)])), jnp.bfloat16),
            pltpu.VMEM((features, LANES), jnp.float32),
            pltpu.VMEM((5, 1, own), jnp.float32),
            pltpu.VMEM((group * ns, 1, own), jnp.float32),
            pltpu.VMEM((1, tokens), jnp.float32),
            pltpu.VMEM((count, 2, tokens), jnp.float32),
            pltpu.VMEM((1, tokens), jnp.float32),
            pltpu.VMEM((16, tokens), jnp.float32),
            dma((planes,)), dma((planes,)),
            dma((planes, half)), dma((planes, half)),
            dma((planes, half)), dma((planes, half)),
            dma((group * ns,)), dma((group * ns,)),
            dma, dma,
            dma((2,)), dma((2,)),
            dma, dma((len(phases), 2)),
        ],
        compiler_params=pltpu.CompilerParams(
            collective_id=0, has_side_effects=True, vmem_limit_bytes=60 * 2**20),
    )(hidden_states.T, norm_gain.reshape(-1, LANES), targets.reshape(1, -1), embedding)
    return loss.reshape(own), mean.reshape(())


def solution(mesh):
    placed = (P("seq", "vocab"), P(), P(("vocab", "seq"), None), P())
    body = functools.partial(local, mesh.shape["vocab"], mesh.shape["seq"])
    return jax.shard_map(
        body, mesh=mesh, in_specs=placed, out_specs=(P("seq"), P()), check_vma=False
    )
```
